32 devices in a mesh: outer: 4 (over y, core), inner: 8 (over z, x).
Axes of the slice: x: 2, y: 2, z: 4, core: 2. Of those that a mesh axis runs over, the one named last changes fastest.
Arguments:
- query_rows: bfloat16 [8192, 1024], P(('outer', 'inner')), may hold values from -6 to 6
- key_rows: bfloat16 [8192, 1024], P(('outer', 'inner')), may hold values from -6 to 6
- value_rows: bfloat16 [8192, 1024], P(('outer', 'inner')), may hold values from -6 to 6
- log_decay: float32 [8, 8192], P(None, ('outer', 'inner')), may hold values from -0.8 to 0, as said below
- grad_out: bfloat16 [8192, 1024], P(('outer', 'inner')), may hold values from -6 to 6
Outputs:
- attended: bfloat16 [8192, 1024], P(('outer', 'inner'))
- grad_queries: bfloat16 [8192, 1024], P(('outer', 'inner'))
- grad_keys: bfloat16 [8192, 1024], P(('outer', 'inner'))
- grad_values: bfloat16 [8192, 1024], P(('outer', 'inner'))
The draws below stay inside these ranges and needn't reach their ends.
Inputs may be any that keep to these rules, and one draw needn't show every extreme that they name: `log_decay`: every entry is negative.
All inputs are finite; a program needn't handle non-finite values.
Results may differ from the reference program's by a relative error of at most 0.0063.
Values sent between devices are 32-bit elements; how exact they have to be, the bound alone decides.
A program may use at most 320 MiB of HBM per device.

```python
import math
import jax
import jax.numpy as jnp
from jax import lax

HALF_HEADS = 8
E = 128
TOK_DEV = 256
SEQUENCE_TOKENS = 8192


def draw_log_decay(key, part):
    random_subkeys = jax.random.split(jax.random.fold_in(key, 17), 7)
    ranking = jax.random.permutation(random_subkeys[0], HALF_HEADS)
    fast_count = HALF_HEADS // 2
    fast_head_flags = ranking < fast_count
    fast_rate = jnp.exp(jax.random.uniform(random_subkeys[1], (HALF_HEADS,), jnp.float32, jnp.log(5.0), jnp.log(50.0))) / SEQUENCE_TOKENS
    slow_rate = jnp.exp(jax.random.uniform(random_subkeys[2], (HALF_HEADS,), jnp.float32, jnp.log(0.05), jnp.log(0.25))) / SEQUENCE_TOKENS
    base_rate = jnp.where(fast_head_flags, fast_rate, slow_rate)
    blocks = SEQUENCE_TOKENS // TOK_DEV
    block_factor = jax.random.uniform(random_subkeys[3], (HALF_HEADS, blocks), jnp.float32, 0.5, 2.0)
    block_factor = jnp.repeat(block_factor, TOK_DEV, axis=1)
    token_factor = jax.random.uniform(random_subkeys[4], (HALF_HEADS, SEQUENCE_TOKENS), jnp.float32, 0.5, 1.5)
    decay_rates = base_rate[:, None] * block_factor * token_factor
    spike_position = jax.random.randint(random_subkeys[5], (HALF_HEADS, 2), 0, SEQUENCE_TOKENS)
    spike_length = jax.random.uniform(random_subkeys[6], (HALF_HEADS, 2), jnp.float32, jnp.log(0.5), jnp.log(0.8))
    token_positions = jnp.arange(SEQUENCE_TOKENS, dtype=jnp.int32)
    spike_flags = token_positions[None, None, :] == spike_position[:, :, None]
    decay_spikes = jnp.sum(jnp.where(spike_flags, spike_length[:, :, None], 0.0), axis=1)
    decay_spikes = jnp.where(fast_head_flags[:, None], 0.0, decay_spikes)
    return (decay_spikes - decay_rates).astype(jnp.float32)


def steps_of(stream_key, shape, cuts, least, largest):
    def one(axis_at, parts):
        draws = jax.random.uniform(jax.random.fold_in(jax.random.fold_in(stream_key, 6), axis_at), (parts,), jnp.float32, least / len(cuts), largest / len(cuts))
        return jnp.repeat(jnp.exp(draws), shape[axis_at] // parts).reshape((-1,) + (1,) * (len(shape) - axis_at - 1))

    factor_of = one(*cuts[0])
    for cut in cuts[1:]:
        factor_of = factor_of * one(*cut)
    return factor_of


def scatter_about(rng, shape, deviation, limit, shards=(), kind=jnp.bfloat16):
    drawn = deviation * jax.random.normal(rng, shape, jnp.float32)
    if shards:
        drawn = drawn * steps_of(rng, shape, shards, -0.22, 0.18)
    return jnp.clip(drawn, -limit, limit).astype(kind)


def setup_inputs(seed: int = 0) -> dict:
    streams_of = jax.random.split(jax.random.key(seed), 6)
    query_rows = scatter_about(streams_of[0], (SEQUENCE_TOKENS, HALF_HEADS * E), 1.0, 6.0, ((0, 32),))
    key_rows = scatter_about(streams_of[1], (SEQUENCE_TOKENS, HALF_HEADS * E), 1.0, 6.0, ((0, 32),))
    value_rows = scatter_about(streams_of[2], (SEQUENCE_TOKENS, HALF_HEADS * E), 1.0, 6.0, ((0, 32),))
    log_decay = draw_log_decay(jax.random.fold_in(streams_of[5], 71), 0)
    grad_out = scatter_about(streams_of[4], (SEQUENCE_TOKENS, HALF_HEADS * E), 1.0, 6.0, ((0, 32),))
    return dict(query_rows=query_rows, key_rows=key_rows, value_rows=value_rows, log_decay=log_decay, grad_out=grad_out)


EPSILON = 1e-06

def causal_decay(running):
    length_rows = running.shape[1]
    row_index = lax.broadcasted_iota(jnp.int32, (length_rows, length_rows), 0)
    col_index = lax.broadcasted_iota(jnp.int32, (length_rows, length_rows), 1)
    causal = (col_index <= row_index)[None]
    gaps = running[:, :, None] - running[:, None, :]
    return jnp.where(causal, jnp.exp(jnp.where(causal, gaps, 0.0)), 0.0)

def block_terms(query_block, key_block, decays, scaling):
    running = jnp.cumsum(decays, axis=1)
    totals = running[:, -1]
    growth = jnp.exp(running).T[:, :, None]
    shrink = jnp.exp(totals[:, None] - running).T[:, :, None]
    query_dec = (query_block.astype(jnp.float32) * growth).astype(jnp.bfloat16)
    key_dec = (key_block.astype(jnp.float32) * shrink).astype(jnp.bfloat16)
    decay_mat = causal_decay(running)
    scores = jnp.einsum('the,she->hts', query_block.astype(jnp.float32), key_block.astype(jnp.float32))
    weights = (scores * scaling * decay_mat).astype(jnp.bfloat16)
    return (totals, growth, shrink, query_dec, key_dec, decay_mat, weights)

def reference(query_rows, key_rows, value_rows, log_decay, grad_out):
    blocks = SEQUENCE_TOKENS // TOK_DEV
    scaling = 1.0 / math.sqrt(E)
    block_shape = (blocks, TOK_DEV, HALF_HEADS, E)
    query_all = query_rows.reshape(block_shape)
    key_all = key_rows.reshape(block_shape)
    value_all = value_rows.reshape(block_shape)
    grad_all = grad_out.reshape(block_shape)
    decay_all = log_decay.reshape(HALF_HEADS, blocks, TOK_DEV).transpose(1, 0, 2)

    def forward_step(carry_state, inputs):
        query_block, key_block, value_block, decays = inputs
        totals, growth, shrink, query_dec, key_dec, decay_mat, weights = block_terms(query_block, key_block, decays, scaling)
        local_state = jnp.einsum('the,thf->hef', key_dec.astype(jnp.float32), value_block.astype(jnp.float32))
        new_state = jnp.exp(totals)[:, None, None] * carry_state + local_state
        return (new_state, carry_state.astype(jnp.bfloat16))
    start_state = jnp.zeros((HALF_HEADS, E, E), jnp.float32)
    _, entering = lax.scan(forward_step, start_state, (query_all, key_all, value_all, decay_all))

    def backward_step(later_state, inputs):
        query_block, key_block, value_block, decays, entering_half, grad_block = inputs
        totals, growth, shrink, query_dec, key_dec, decay_mat, weights = block_terms(query_block, key_block, decays, scaling)
        value_float = value_block.astype(jnp.float32)
        entering_float = entering_half.astype(jnp.float32)
        mixed = jnp.einsum('hts,shf->thf', weights.astype(jnp.float32), value_float)
        mixed = mixed + scaling * jnp.einsum('the,hef->thf', query_dec.astype(jnp.float32), entering_float)
        inverse = lax.rsqrt(lax.optimization_barrier(jnp.mean(mixed * mixed, axis=2, keepdims=True)) + EPSILON)
        normed = mixed * inverse
        grad_normed = grad_block.astype(jnp.float32)
        grad_mixed = (inverse * (grad_normed - normed * lax.optimization_barrier(jnp.mean(grad_normed * normed, axis=2, keepdims=True)))).astype(jnp.bfloat16)
        grad_float = grad_mixed.astype(jnp.float32)
        back_state = scaling * jnp.einsum('the,thf->hef', query_dec.astype(jnp.float32), grad_float)
        leaving_float = later_state.astype(jnp.bfloat16).astype(jnp.float32)
        grad_prob = jnp.einsum('thf,shf->hts', grad_float, value_float)
        grad_score = (grad_prob * scaling * decay_mat).astype(jnp.bfloat16).astype(jnp.float32)
        grad_q = jnp.einsum('hts,she->the', grad_score, key_block.astype(jnp.float32))
        grad_q = grad_q + scaling * growth * jnp.einsum('thf,hef->the', grad_float, entering_float)
        grad_k = jnp.einsum('hts,the->she', grad_score, query_block.astype(jnp.float32))
        grad_k = grad_k + shrink * jnp.einsum('shf,hef->she', value_float, leaving_float)
        grad_v = jnp.einsum('hts,thf->shf', weights.astype(jnp.float32), grad_float)
        grad_v = grad_v + jnp.einsum('she,hef->shf', key_dec.astype(jnp.float32), leaving_float)
        new_later = jnp.exp(totals)[:, None, None] * later_state + back_state
        return (new_later, (normed.astype(jnp.bfloat16), grad_q.astype(jnp.bfloat16), grad_k.astype(jnp.bfloat16), grad_v.astype(jnp.bfloat16)))
    _, results = lax.scan(backward_step, start_state, (query_all, key_all, value_all, decay_all, entering, grad_all), reverse=True)
    attended, grad_queries, grad_keys, grad_values = [piece.reshape(SEQUENCE_TOKENS, HALF_HEADS * E) for piece in results]
    return (attended, grad_queries, grad_keys, grad_values)
```

```python
import functools
import math

import jax
import jax.numpy as jnp
from jax import lax
from jax.experimental import pallas as pl
from jax.experimental.pallas import tpu as pltpu
from jax.sharding import PartitionSpec as P

EPSILON = 1e-06
F32 = jnp.float32
BF16 = jnp.bfloat16
MESH = pl.DeviceIdType.MESH


def dot(a, b, da, db):
    return lax.dot_general(a, b, (((da,), (db,)), ((), ())), preferred_element_type=F32)


def kernel(outer_size, inner_size, q_ref, k_ref, v_ref, decay_ref, g_ref,
           att_ref, gq_ref, gk_ref, gv_ref,
           run_ref, col_ref, tot_ref, fac_ref, facs_ref, dec_ref, w_ref, kd_ref, mix_ref, gm_ref,
           send1, recv1, out1, ret1, send2, recv2, out2, ret2, ent_ref, gkl_ref, gvl_ref,
           send_sems, recv_sems):
    n = outer_size * inner_size
    heads, tokens = decay_ref.shape
    size = q_ref.shape[1] // heads
    scaling = 1.0 / math.sqrt(size)
    per_head = n // heads
    rows = size // per_head
    place_o, place_i = lax.axis_index("outer"), lax.axis_index("inner")
    me = place_o * inner_size + place_i

    def partner(i):
        t = i // outer_size
        step_o = (i % outer_size + 1) % outer_size
        step_i = inner_size // 2 + ((t + 1) // 2) * (2 * (t % 2) - 1) + inner_size
        return (place_o + step_o) % outer_size, (place_i + step_i) % inner_size

    def each_partner(act):
        def turn(i, carry):
            act(*partner(i))
            return carry
        lax.fori_loop(0, n - 1, turn, 0)

    def exchange(source_of, target, phase):
        def act(o, i):
            pltpu.make_async_remote_copy(
                src_ref=source_of(o * inner_size + i), dst_ref=target.at[me],
                send_sem=send_sems.at[phase], recv_sem=recv_sems.at[phase],
                device_id=(o, i), device_id_type=MESH).start()
        each_partner(act)

    def drain(buffer, sem):
        part = buffer.at[pl.ds(0, n - 1)]
        pltpu.make_async_copy(part, part, sem).wait()

    def each_head(act):
        def turn(i, carry):
            act(2 * i)
            act(2 * i + 1)
            return carry
        lax.fori_loop(0, heads // 2, turn, 0)

    def span(h):
        return pl.ds(pl.multiple_of(h * size, size), size)

    def put_state(target, h, state):
        if rows % 8 == 0:
            target[pl.ds(h * per_head, per_head)] = state.reshape(per_head, rows, size)
        else:
            for p in range(per_head):
                target[h * per_head + p] = state[p * rows:(p + 1) * rows]

    def get_state(source, h):
        if rows % 8 == 0:
            return source[pl.ds(h * per_head, per_head)].reshape(size, size)
        return jnp.concatenate([source[h * per_head + p] for p in range(per_head)], axis=0)

    barrier = pltpu.get_barrier_semaphore()
    each_partner(lambda o, i: pl.semaphore_signal(barrier, inc=1, device_id=(o, i), device_id_type=MESH))

    running = decay_ref[...]
    lane = lax.broadcasted_iota(jnp.int32, (heads, tokens), 1)
    shift = 1
    while shift < tokens:
        running = running + jnp.where(lane >= shift, pltpu.roll(running, shift, 1), 0.0)
        shift *= 2
    run_ref[...] = running
    for h in range(heads):
        row = running[h:h + 1]
        col_ref[h] = jnp.broadcast_to(row, (size, tokens)).T
        total = jnp.broadcast_to(row[:, tokens - 1:], (1, size))
        tot_ref[h] = total
        fac_ref[h] = jnp.exp(total)

    def state_of(h):
        cols = span(h)
        shrink = jnp.exp(tot_ref[h] - col_ref[h])
        key_dec = (k_ref[:, cols].astype(F32) * shrink).astype(BF16)
        kd_ref[:, cols] = key_dec
        put_state(send1, h, dot(key_dec, v_ref[:, cols], 0, 0))

    each_head(state_of)
    pl.semaphore_wait(barrier, n - 1)
    exchange(lambda c: fac_ref.at[c // per_head], facs_ref, 4)
    exchange(lambda c: send1.at[c], recv1, 0)
    facs_ref[me] = fac_ref[me // per_head]
    recv1[me] = send1[me]

    t_index = lax.broadcasted_iota(jnp.int32, (tokens, tokens), 0)
    s_index = lax.broadcasted_iota(jnp.int32, (tokens, tokens), 1)
    causal = s_index <= t_index

    def local_mix(h):
        cols = span(h)
        column = jnp.concatenate([col_ref[h]] * (tokens // size), axis=1)
        gaps = column - run_ref[pl.ds(h, 1)]
        decay = jnp.where(causal, jnp.exp(jnp.where(causal, gaps, 0.0)), 0.0) * scaling
        dec_ref[h] = decay
        weights = (dot(q_ref[:, cols], k_ref[:, cols], 1, 1) * decay).astype(BF16)
        w_ref[h] = weights
        mix_ref[:, cols] = dot(weights, v_ref[:, cols], 1, 0)

    each_head(local_mix)

    def scan(source, target, backward):
        def turn(i, state):
            at = n - 1 - i if backward else i
            target[at] = state
            return facs_ref[at] * state + source[at]
        lax.fori_loop(0, n, turn, jnp.zeros((rows, size), F32))

    drain(facs_ref, recv_sems.at[4])
    drain(recv1, recv_sems.at[0])
    scan(recv1, out1, False)
    exchange(lambda c: out1.at[c], ret1, 1)
    ret1[me] = out1[me]
    drain(ret1, recv_sems.at[1])

    def mix(h):
        cols = span(h)
        entering = get_state(ret1, h).astype(BF16)
        ent_ref[h] = entering
        growth = jnp.exp(col_ref[h])
        query_dec = (q_ref[:, cols].astype(F32) * growth).astype(BF16)
        mixed = mix_ref[:, cols] + scaling * dot(query_dec, entering, 1, 0)
        inverse = lax.rsqrt(jnp.mean(mixed * mixed, axis=1, keepdims=True) + EPSILON)
        normed = mixed * inverse
        att_ref[:, cols] = normed.astype(BF16)
        g = g_ref[:, cols].astype(F32)
        grad_mixed = (inverse * (g - normed * jnp.mean(g * normed, axis=1, keepdims=True))).astype(BF16)
        gm_ref[:, cols] = grad_mixed
        put_state(send2, h, scaling * dot(query_dec, grad_mixed, 0, 0))

    each_head(mix)
    exchange(lambda c: send2.at[c], recv2, 2)
    recv2[me] = send2[me]

    def local_grads(h):
        cols = span(h)
        grad_mixed = gm_ref[:, cols]
        grad_score = (dot(grad_mixed, v_ref[:, cols], 1, 1) * dec_ref[h]).astype(BF16)
        far = (scaling * jnp.exp(col_ref[h])) * dot(grad_mixed, ent_ref[h], 1, 1)
        gq_ref[:, cols] = (dot(grad_score, k_ref[:, cols], 1, 0) + far).astype(BF16)
        gkl_ref[:, cols] = dot(grad_score, q_ref[:, cols], 0, 0)
        gvl_ref[:, cols] = dot(w_ref[h], grad_mixed, 0, 0)

    each_head(local_grads)
    drain(recv2, recv_sems.at[2])
    scan(recv2, out2, True)
    exchange(lambda c: out2.at[c], ret2, 3)
    ret2[me] = out2[me]
    drain(ret2, recv_sems.at[3])

    def far_grads(h):
        cols = span(h)
        leaving = get_state(ret2, h).astype(BF16)
        shrink = jnp.exp(tot_ref[h] - col_ref[h])
        gk_ref[:, cols] = (gkl_ref[:, cols] + shrink * dot(v_ref[:, cols], leaving, 1, 1)).astype(BF16)
        gv_ref[:, cols] = (gvl_ref[:, cols] + dot(kd_ref[:, cols], leaving, 1, 0)).astype(BF16)

    each_head(far_grads)
    drain(facs_ref, send_sems.at[4])
    for phase, buffer in enumerate((send1, out1, send2, out2)):
        drain(buffer, send_sems.at[phase])


def body(outer_size, inner_size, query_rows, key_rows, value_rows, log_decay, grad_out):
    n = outer_size * inner_size
    heads, tokens = log_decay.shape
    wide = query_rows.shape[1]
    size = wide // heads
    rows = heads * size // n
    pieces = pltpu.VMEM((n, rows, size), F32)
    vmem = pl.BlockSpec(memory_space=pltpu.VMEM)
    return pl.pallas_call(
        functools.partial(kernel, outer_size, inner_size),
        out_shape=[jax.ShapeDtypeStruct((tokens, wide), BF16)] * 4,
        in_specs=[vmem] * 5,
        out_specs=[vmem] * 4,
        scratch_shapes=[
            pltpu.VMEM((heads, tokens), F32),
            pltpu.VMEM((heads, tokens, size), F32),
            pltpu.VMEM((heads, 1, size), F32),
            pltpu.VMEM((heads, 1, size), F32),
            pltpu.VMEM((n, 1, size), F32),
            pltpu.VMEM((heads, tokens, tokens), F32),
            pltpu.VMEM((heads, tokens, tokens), BF16),
            pltpu.VMEM((tokens, wide), BF16),
            pltpu.VMEM((tokens, wide), F32),
            pltpu.VMEM((tokens, wide), BF16),
            pieces, pieces, pieces, pieces, pieces, pieces, pieces, pieces,
            pltpu.VMEM((heads, size, size), BF16),
            pltpu.VMEM((tokens, wide), F32),
            pltpu.VMEM((tokens, wide), F32),
            pltpu.SemaphoreType.DMA((5,)),
            pltpu.SemaphoreType.DMA((5,)),
        ],
        compiler_params=pltpu.CompilerParams(
            collective_id=0, has_side_effects=True, vmem_limit_bytes=48 * 1024 * 1024),
    )(query_rows, key_rows, value_rows, log_decay, grad_out)


def solution(mesh):
    both = ("outer", "inner")
    row_spec = P(both, None)
    return jax.shard_map(
        functools.partial(body, mesh.shape["outer"], mesh.shape["inner"]),
        mesh=mesh,
        in_specs=(row_spec, row_spec, row_spec, P(None, both), row_spec),
        out_specs=(row_spec,) * 4,
        check_vma=False,
    )
```

```python
import functools
import math

import jax
import jax.numpy as jnp
from jax import lax
from jax.experimental import pallas as pl
from jax.experimental.pallas import tpu as pltpu
from jax.sharding import PartitionSpec as P

EPSILON = 1e-06
F32 = jnp.float32
BF16 = jnp.bfloat16
MESH = pl.DeviceIdType.MESH
PARTS = 2


def dot(a, b, da, db):
    return lax.dot_general(a, b, (((da,), (db,)), ((), ())), preferred_element_type=F32)


def kernel(outer_size, inner_size, parts, q_hbm, k_hbm, v_hbm, decay_hbm, g_hbm,
           att_ref, gq_ref, gk_ref, gv_ref,
           q_ref, k_ref, v_ref, decay_ref, g_ref,
           run_ref, col_ref, tot_ref, fac_ref, facs_ref, dec_ref, w_ref, kd_ref, mix_ref, gm_ref,
           send1, recv1, out1, ret1, agg1, send2, recv2, out2, ret2, agg2, ent_ref, gkl_ref, gvl_ref,
           load_sems, fac_sems, send_sems, recv_sems):
    n = outer_size * inner_size
    half_inner = inner_size // 2
    count = n // 2
    heads, tokens = decay_ref.shape
    size = q_ref.shape[1] // heads
    scaling = 1.0 / math.sqrt(size)
    per_head = count // heads
    rows = size // (per_head * parts)
    place_o, place_i = lax.axis_index("outer"), lax.axis_index("inner")
    half = place_i // half_inner
    me = place_o * inner_size + place_i
    seat = place_o * half_inner + place_i % half_inner

    loads = [pltpu.make_async_copy(source, target, load_sems.at[at]) for at, (source, target) in enumerate(
        ((decay_hbm, decay_ref), (k_hbm, k_ref), (v_hbm, v_ref), (q_hbm, q_ref), (g_hbm, g_ref)))]
    for load in loads:
        load.start()

    def everyone(act):
        def turn(i, carry):
            at = (me + 1 + i) % n
            act(at // inner_size, at % inner_size)
            return carry
        lax.fori_loop(0, n - 1, turn, 0)

    def seat_of(o, i):
        return o * half_inner + i % half_inner

    barrier = pltpu.get_barrier_semaphore()
    everyone(lambda o, i: pl.semaphore_signal(barrier, inc=1, device_id=(o, i), device_id_type=MESH))

    def exchange(source, target, phase, part):
        def turn(i, carry):
            step = i + 1
            o = (place_o + step % outer_size) % outer_size
            i = half * half_inner + (place_i % half_inner + step // outer_size) % half_inner
            pltpu.make_async_remote_copy(
                src_ref=source.at[part, seat_of(o, i)], dst_ref=target.at[part, seat],
                send_sem=send_sems.at[phase, part], recv_sem=recv_sems.at[phase, part],
                device_id=(o, i), device_id_type=MESH).start()
            return carry
        lax.fori_loop(0, count - 1, turn, 0)

    def across(sums, phase, part):
        pltpu.make_async_remote_copy(
            src_ref=sums.at[part, half], dst_ref=sums.at[part, half],
            send_sem=send_sems.at[phase, part], recv_sem=recv_sems.at[phase, part],
            device_id=(place_o, (place_i + half_inner) % inner_size), device_id_type=MESH).start()

    def drain(piece, sem):
        pltpu.make_async_copy(piece, piece, sem).wait()

    def others(buffer, part):
        return buffer.at[part, pl.ds(0, count - 1)]

    def each_head(act):
        def turn(i, carry):
            act(2 * i)
            act(2 * i + 1)
            return carry
        lax.fori_loop(0, heads // 2, turn, 0)

    def span(h):
        return pl.ds(pl.multiple_of(h * size, size), size)

    def put_state(target, h, state):
        for p in range(per_head):
            for part in range(parts):
                first = (p * parts + part) * rows
                target[part, h * per_head + p] = state[first:first + rows]

    def get_state(source, h):
        return jnp.concatenate(
            [source[part, h * per_head + p] for p in range(per_head) for part in range(parts)], axis=0)

    loads[0].wait()
    running = decay_ref[...]
    lane = lax.broadcasted_iota(jnp.int32, (heads, tokens), 1)
    shift = 1
    while shift < tokens:
        running = running + jnp.where(lane >= shift, pltpu.roll(running, shift, 1), 0.0)
        shift *= 2
    run_ref[...] = running
    for h in range(heads):
        row = running[h:h + 1]
        col_ref[h] = jnp.broadcast_to(row, (size, tokens)).T
        total = jnp.broadcast_to(row[:, tokens - 1:], (1, size))
        tot_ref[h] = total
        fac_ref[h] = jnp.exp(total)
    loads[1].wait()
    loads[2].wait()

    def state_of(h):
        cols = span(h)
        shrink = jnp.exp(tot_ref[h] - col_ref[h])
        key_dec = (k_ref[:, cols].astype(F32) * shrink).astype(BF16)
        kd_ref[:, cols] = key_dec
        put_state(send1, h, dot(key_dec, v_ref[:, cols], 0, 0))

    each_head(state_of)
    pl.semaphore_wait(barrier, n - 1)

    def send_factor(o, i):
        pltpu.make_async_remote_copy(
            src_ref=fac_ref.at[seat_of(o, i) // per_head], dst_ref=facs_ref.at[me],
            send_sem=fac_sems.at[0], recv_sem=fac_sems.at[1],
            device_id=(o, i), device_id_type=MESH).start()

    exchange(send1, recv1, 0, 0)
    everyone(send_factor)
    for part in range(1, parts):
        exchange(send1, recv1, 0, part)
    facs_ref[me] = fac_ref[seat // per_head]
    for part in range(parts):
        recv1[part, seat] = send1[part, seat]

    t_index = lax.broadcasted_iota(jnp.int32, (tokens, tokens), 0)
    s_index = lax.broadcasted_iota(jnp.int32, (tokens, tokens), 1)
    causal = s_index <= t_index

    def local_mix(h):
        cols = span(h)
        column = jnp.concatenate([col_ref[h]] * (tokens // size), axis=1)
        gaps = column - run_ref[pl.ds(h, 1)]
        decay = jnp.where(causal, jnp.exp(jnp.where(causal, gaps, 0.0)), 0.0) * scaling
        dec_ref[h] = decay
        weights = (dot(q_ref[:, cols], k_ref[:, cols], 1, 1) * decay).astype(BF16)
        w_ref[h] = weights
        mix_ref[:, cols] = dot(weights, v_ref[:, cols], 1, 0)

    def group_sums(source, sums, part, backward):
        def group(o, carry):
            state = jnp.zeros((rows, size), F32)
            for step in range(half_inner):
                at = half_inner - 1 - step if backward else step
                factor = facs_ref[o * inner_size + half * half_inner + at]
                state = factor * state + source[part, o * half_inner + at]
            sums[part, half, o] = state
            return carry
        lax.fori_loop(0, outer_size, group, 0)

    def scan(source, sums, target, part, backward):
        order = (1, 0) if backward else (0, 1)

        def group(turn, carry):
            o = outer_size - 1 - turn if backward else turn
            entry = []
            for side in order:
                entry.append(carry)
                factor = facs_ref[o * inner_size + side * half_inner]
                for step in range(1, half_inner):
                    factor = factor * facs_ref[o * inner_size + side * half_inner + step]
                carry = factor * carry + sums[part, side, o]
            state = jnp.where(half == order[0], entry[0], entry[1])
            for step in range(half_inner):
                at = half_inner - 1 - step if backward else step
                target[part, o * half_inner + at] = state
                factor = facs_ref[o * inner_size + half * half_inner + at]
                state = factor * state + source[part, o * half_inner + at]
            return carry
        lax.fori_loop(0, outer_size, group, jnp.zeros((rows, size), F32))

    def carried(source, sums, target, result, phase, backward):
        for part in range(parts):
            drain(others(source, part), recv_sems.at[phase, part])
            group_sums(source, sums, part, backward)
            across(sums, phase + 1, part)
        for part in range(parts):
            drain(sums.at[part, 1 - half], recv_sems.at[phase + 1, part])
            scan(source, sums, target, part, backward)
            exchange(target, result, phase + 2, part)
            result[part, seat] = target[part, seat]

    loads[3].wait()
    drain(facs_ref.at[pl.ds(0, n - 1)], fac_sems.at[1])
    each_head(local_mix)
    carried(recv1, agg1, out1, ret1, 0, False)
    loads[4].wait()
    for part in range(parts):
        drain(others(ret1, part), recv_sems.at[2, part])

    def mix(h):
        cols = span(h)
        entering = get_state(ret1, h).astype(BF16)
        ent_ref[h] = entering
        growth = jnp.exp(col_ref[h])
        query_dec = (q_ref[:, cols].astype(F32) * growth).astype(BF16)
        mixed = mix_ref[:, cols] + scaling * dot(query_dec, entering, 1, 0)
        inverse = lax.rsqrt(jnp.mean(mixed * mixed, axis=1, keepdims=True) + EPSILON)
        normed = mixed * inverse
        att_ref[:, cols] = normed.astype(BF16)
        g = g_ref[:, cols].astype(F32)
        grad_mixed = (inverse * (g - normed * jnp.mean(g * normed, axis=1, keepdims=True))).astype(BF16)
        gm_ref[:, cols] = grad_mixed
        put_state(send2, h, scaling * dot(query_dec, grad_mixed, 0, 0))

    each_head(mix)
    for part in range(parts):
        exchange(send2, recv2, 3, part)
    for part in range(parts):
        recv2[part, seat] = send2[part, seat]

    def local_grads(h):
        cols = span(h)
        grad_mixed = gm_ref[:, cols]
        grad_score = (dot(grad_mixed, v_ref[:, cols], 1, 1) * dec_ref[h]).astype(BF16)
        far = (scaling * jnp.exp(col_ref[h])) * dot(grad_mixed, ent_ref[h], 1, 1)
        gq_ref[:, cols] = (dot(grad_score, k_ref[:, cols], 1, 0) + far).astype(BF16)
        gkl_ref[:, cols] = dot(grad_score, q_ref[:, cols], 0, 0)
        gvl_ref[:, cols] = dot(w_ref[h], grad_mixed, 0, 0)

    each_head(local_grads)
    carried(recv2, agg2, out2, ret2, 3, True)
    for part in range(parts):
        drain(others(ret2, part), recv_sems.at[5, part])

    def far_grads(h):
        cols = span(h)
        leaving = get_state(ret2, h).astype(BF16)
        shrink = jnp.exp(tot_ref[h] - col_ref[h])
        gk_ref[:, cols] = (gkl_ref[:, cols] + shrink * dot(v_ref[:, cols], leaving, 1, 1)).astype(BF16)
        gv_ref[:, cols] = (gvl_ref[:, cols] + dot(kd_ref[:, cols], leaving, 1, 0)).astype(BF16)

    each_head(far_grads)
    drain(facs_ref.at[pl.ds(0, n - 1)], fac_sems.at[0])
    for part in range(parts):
        for phase, buffer in ((0, send1), (2, out1), (3, send2), (5, out2)):
            drain(others(buffer, part), send_sems.at[phase, part])
        drain(agg1.at[part, half], send_sems.at[1, part])
        drain(agg2.at[part, half], send_sems.at[4, part])


def store(*refs):
    sources, targets, sems = refs[:4], refs[4:8], refs[8]
    copies = [pltpu.make_async_copy(s, t, sems.at[at]) for at, (s, t) in enumerate(zip(sources, targets))]
    for copy in copies:
        copy.start()
    for copy in copies:
        copy.wait()


def body(outer_size, inner_size, query_rows, key_rows, value_rows, log_decay, grad_out):
    n = outer_size * inner_size
    heads, tokens = log_decay.shape
    wide = query_rows.shape[1]
    size = wide // heads
    count = n // 2
    chunk = heads * size // count
    parts = PARTS if chunk % (8 * PARTS) == 0 else 1
    rows = chunk // parts
    pieces = pltpu.VMEM((parts, count, rows, size), F32)
    sums = pltpu.VMEM((parts, 2, outer_size, rows, size), F32)
    vmem = pl.BlockSpec(memory_space=pltpu.VMEM)
    hbm = pl.BlockSpec(memory_space=pltpu.HBM)
    row_block = pltpu.VMEM((tokens, wide), BF16)
    outs = [jax.ShapeDtypeStruct((tokens, wide), BF16)] * 4
    results = pl.pallas_call(
        functools.partial(kernel, outer_size, inner_size, parts),
        out_shape=outs,
        in_specs=[hbm] * 5,
        out_specs=[vmem] * 4,
        scratch_shapes=[
            row_block, row_block, row_block, pltpu.VMEM((heads, tokens), F32), row_block,
            pltpu.VMEM((heads, tokens), F32),
            pltpu.VMEM((heads, tokens, size), F32),
            pltpu.VMEM((heads, 1, size), F32),
            pltpu.VMEM((heads, 1, size), F32),
            pltpu.VMEM((n, 1, size), F32),
            pltpu.VMEM((heads, tokens, tokens), F32),
            pltpu.VMEM((heads, tokens, tokens), BF16),
            row_block,
            pltpu.VMEM((tokens, wide), F32),
            row_block,
            pieces, pieces, pieces, pieces, sums, pieces, pieces, pieces, pieces, sums,
            pltpu.VMEM((heads, size, size), BF16),
            pltpu.VMEM((tokens, wide), F32),
            pltpu.VMEM((tokens, wide), F32),
            pltpu.SemaphoreType.DMA((5,)),
            pltpu.SemaphoreType.DMA((2,)),
            pltpu.SemaphoreType.DMA((6, parts)),
            pltpu.SemaphoreType.DMA((6, parts)),
        ],
        compiler_params=pltpu.CompilerParams(
            collective_id=0, has_side_effects=True, vmem_limit_bytes=40 * 1024 * 1024),
    )(query_rows, key_rows, value_rows, log_decay, grad_out)
    return pl.pallas_call(
        store,
        out_shape=outs,
        in_specs=[vmem] * 4,
        out_specs=[hbm] * 4,
        scratch_shapes=[pltpu.SemaphoreType.DMA((4,))],
        compiler_params=pltpu.CompilerParams(vmem_limit_bytes=8 * 1024 * 1024),
    )(*results)


def solution(mesh):
    both = ("outer", "inner")
    row_spec = P(both, None)
    return jax.shard_map(
        functools.partial(body, mesh.shape["outer"], mesh.shape["inner"]),
        mesh=mesh,
        in_specs=(row_spec, row_spec, row_spec, P(None, both), row_spec),
        out_specs=(row_spec,) * 4,
        check_vma=False,
    )
```

```python
import functools
import math

import jax
import jax.numpy as jnp
from jax import lax
from jax.experimental import pallas as pl
from jax.experimental.pallas import tpu as pltpu
from jax.sharding import PartitionSpec as P

EPSILON = 1e-06
F32 = jnp.float32
BF16 = jnp.bfloat16
MESH = pl.DeviceIdType.MESH
PARTS = 4


def dot(a, b, da, db):
    return lax.dot_general(a, b, (((da,), (db,)), ((), ())), preferred_element_type=F32)


def kernel(outer_size, inner_size, parts, q_hbm, k_hbm, v_hbm, decay_hbm, g_hbm,
           att_ref, gq_ref, gk_ref, gv_ref,
           q_ref, k_ref, v_ref, decay_ref, g_ref,
           run_ref, col_ref, tot_ref, fac_ref, facs_ref, dec_ref, w_ref, kd_ref, mix_ref, gm_ref,
           send1, recv1, out1, ret1, agg1, send2, recv2, out2, ret2, agg2, ent_ref, gkl_ref, gvl_ref,
           load_sems, fac_sems, send_sems, recv_sems):
    n = outer_size * inner_size
    half_inner = inner_size // 2
    count = n // 2
    heads, tokens = decay_ref.shape
    size = q_ref.shape[1] // heads
    scaling = 1.0 / math.sqrt(size)
    per_head = count // heads
    rows = size // (per_head * parts)
    place_o, place_i = lax.axis_index("outer"), lax.axis_index("inner")
    half = place_i // half_inner
    me = place_o * inner_size + place_i
    seat = place_o * half_inner + place_i % half_inner

    loads = [pltpu.make_async_copy(source, target, load_sems.at[at]) for at, (source, target) in enumerate(
        ((decay_hbm, decay_ref), (k_hbm, k_ref), (v_hbm, v_ref), (q_hbm, q_ref), (g_hbm, g_ref)))]
    for load in loads:
        load.start()

    def everyone(act):
        def turn(i, carry):
            at = (me + 1 + i) % n
            act(at // inner_size, at % inner_size)
            return carry
        lax.fori_loop(0, n - 1, turn, 0)

    def seat_of(o, i):
        return o * half_inner + i % half_inner

    barrier = pltpu.get_barrier_semaphore()
    everyone(lambda o, i: pl.semaphore_signal(barrier, inc=1, device_id=(o, i), device_id_type=MESH))

    def exchange(source, target, phase, part):
        def turn(i, carry):
            step = i + 1
            o = (place_o + step % outer_size) % outer_size
            i = half * half_inner + (place_i % half_inner + step // outer_size) % half_inner
            pltpu.make_async_remote_copy(
                src_ref=source.at[part, seat_of(o, i)], dst_ref=target.at[part, seat],
                send_sem=send_sems.at[phase, part], recv_sem=recv_sems.at[phase, part],
                device_id=(o, i), device_id_type=MESH).start()
            return carry
        lax.fori_loop(0, count - 1, turn, 0)

    def across(sums, phase, part):
        pltpu.make_async_remote_copy(
            src_ref=sums.at[part, half], dst_ref=sums.at[part, half],
            send_sem=send_sems.at[phase, part], recv_sem=recv_sems.at[phase, part],
            device_id=(place_o, (place_i + half_inner) % inner_size), device_id_type=MESH).start()

    def drain(piece, sem):
        pltpu.make_async_copy(piece, piece, sem).wait()

    def others(buffer, part):
        return buffer.at[part, pl.ds(0, count - 1)]

    def each_head(act):
        def turn(i, carry):
            act(2 * i)
            act(2 * i + 1)
            return carry
        lax.fori_loop(0, heads // 2, turn, 0)

    def span(h):
        return pl.ds(pl.multiple_of(h * size, size), size)

    def put_state(target, h, state):
        for p in range(per_head):
            for part in range(parts):
                first = (p * parts + part) * rows
                target[part, h * per_head + p] = state[first:first + rows]

    def get_state(source, h):
        return jnp.concatenate(
            [source[part, h * per_head + p] for p in range(per_head) for part in range(parts)], axis=0)

    loads[0].wait()
    running = decay_ref[...]
    lane = lax.broadcasted_iota(jnp.int32, (heads, tokens), 1)
    shift = 1
    while shift < tokens:
        running = running + jnp.where(lane >= shift, pltpu.roll(running, shift, 1), 0.0)
        shift *= 2
    run_ref[...] = running
    for h in range(heads):
        row = running[h:h + 1]
        col_ref[h] = jnp.broadcast_to(row, (size, tokens)).T
        total = jnp.broadcast_to(row[:, tokens - 1:], (1, size))
        tot_ref[h] = total
        fac_ref[h] = jnp.exp(total)
    loads[1].wait()
    loads[2].wait()

    def state_of(h):
        cols = span(h)
        shrink = jnp.exp(tot_ref[h] - col_ref[h])
        key_dec = (k_ref[:, cols].astype(F32) * shrink).astype(BF16)
        kd_ref[:, cols] = key_dec
        put_state(send1, h, dot(key_dec, v_ref[:, cols], 0, 0))

    each_head(state_of)
    pl.semaphore_wait(barrier, n - 1)

    def send_factor(o, i):
        pltpu.make_async_remote_copy(
            src_ref=fac_ref.at[seat_of(o, i) // per_head], dst_ref=facs_ref.at[me],
            send_sem=fac_sems.at[0], recv_sem=fac_sems.at[1],
            device_id=(o, i), device_id_type=MESH).start()

    exchange(send1, recv1, 0, 0)
    everyone(send_factor)
    for part in range(1, parts):
        exchange(send1, recv1, 0, part)
    facs_ref[me] = fac_ref[seat // per_head]
    for part in range(parts):
        recv1[part, seat] = send1[part, seat]

    t_index = lax.broadcasted_iota(jnp.int32, (tokens, tokens), 0)
    s_index = lax.broadcasted_iota(jnp.int32, (tokens, tokens), 1)
    causal = s_index <= t_index

    def local_mix(h):
        cols = span(h)
        column = jnp.concatenate([col_ref[h]] * (tokens // size), axis=1)
        gaps = column - run_ref[pl.ds(h, 1)]
        decay = jnp.where(causal, jnp.exp(jnp.where(causal, gaps, 0.0)), 0.0) * scaling
        dec_ref[h] = decay
        weights = (dot(q_ref[:, cols], k_ref[:, cols], 1, 1) * decay).astype(BF16)
        w_ref[h] = weights
        mix_ref[:, cols] = dot(weights, v_ref[:, cols], 1, 0)

    def group_sums(source, sums, part, backward):
        def group(o, carry):
            state = jnp.zeros((rows, size), F32)
            for step in range(half_inner):
                at = half_inner - 1 - step if backward else step
                factor = facs_ref[o * inner_size + half * half_inner + at]
                state = factor * state + source[part, o * half_inner + at]
            sums[part, half, o] = state
            return carry
        lax.fori_loop(0, outer_size, group, 0)

    def scan(source, sums, target, part, backward):
        order = (1, 0) if backward else (0, 1)

        def group(turn, carry):
            o = outer_size - 1 - turn if backward else turn
            entry = []
            for side in order:
                entry.append(carry)
                factor = facs_ref[o * inner_size + side * half_inner]
                for step in range(1, half_inner):
                    factor = factor * facs_ref[o * inner_size + side * half_inner + step]
                carry = factor * carry + sums[part, side, o]
            state = jnp.where(half == order[0], entry[0], entry[1])
            for step in range(half_inner):
                at = half_inner - 1 - step if backward else step
                target[part, o * half_inner + at] = state
                factor = facs_ref[o * inner_size + half * half_inner + at]
                state = factor * state + source[part, o * half_inner + at]
            return carry
        lax.fori_loop(0, outer_size, group, jnp.zeros((rows, size), F32))

    def carried(source, sums, target, result, phase, backward):
        for part in range(parts):
            drain(others(source, part), recv_sems.at[phase, part])
            group_sums(source, sums, part, backward)
            across(sums, phase + 1, part)
        for part in range(parts):
            drain(sums.at[part, 1 - half], recv_sems.at[phase + 1, part])
            scan(source, sums, target, part, backward)
            exchange(target, result, phase + 2, part)
            result[part, seat] = target[part, seat]

    loads[3].wait()
    drain(facs_ref.at[pl.ds(0, n - 1)], fac_sems.at[1])
    each_head(local_mix)
    carried(recv1, agg1, out1, ret1, 0, False)
    loads[4].wait()
    for part in range(parts):
        drain(others(ret1, part), recv_sems.at[2, part])

    def mix(h):
        cols = span(h)
        entering = get_state(ret1, h).astype(BF16)
        ent_ref[h] = entering
        growth = jnp.exp(col_ref[h])
        query_dec = (q_ref[:, cols].astype(F32) * growth).astype(BF16)
        mixed = mix_ref[:, cols] + scaling * dot(query_dec, entering, 1, 0)
        inverse = lax.rsqrt(jnp.mean(mixed * mixed, axis=1, keepdims=True) + EPSILON)
        normed = mixed * inverse
        att_ref[:, cols] = normed.astype(BF16)
        g = g_ref[:, cols].astype(F32)
        grad_mixed = (inverse * (g - normed * jnp.mean(g * normed, axis=1, keepdims=True))).astype(BF16)
        gm_ref[:, cols] = grad_mixed
        put_state(send2, h, scaling * dot(query_dec, grad_mixed, 0, 0))

    each_head(mix)
    for part in range(parts):
        exchange(send2, recv2, 3, part)
    for part in range(parts):
        recv2[part, seat] = send2[part, seat]

    def local_grads(h):
        cols = span(h)
        grad_mixed = gm_ref[:, cols]
        grad_score = (dot(grad_mixed, v_ref[:, cols], 1, 1) * dec_ref[h]).astype(BF16)
        far = (scaling * jnp.exp(col_ref[h])) * dot(grad_mixed, ent_ref[h], 1, 1)
        gq_ref[:, cols] = (dot(grad_score, k_ref[:, cols], 1, 0) + far).astype(BF16)
        gkl_ref[:, cols] = dot(grad_score, q_ref[:, cols], 0, 0)
        gvl_ref[:, cols] = dot(w_ref[h], grad_mixed, 0, 0)

    each_head(local_grads)
    carried(recv2, agg2, out2, ret2, 3, True)
    for part in range(parts):
        drain(others(ret2, part), recv_sems.at[5, part])

    def far_grads(h):
        cols = span(h)
        leaving = get_state(ret2, h).astype(BF16)
        shrink = jnp.exp(tot_ref[h] - col_ref[h])
        gk_ref[:, cols] = (gkl_ref[:, cols] + shrink * dot(v_ref[:, cols], leaving, 1, 1)).astype(BF16)
        gv_ref[:, cols] = (gvl_ref[:, cols] + dot(kd_ref[:, cols], leaving, 1, 0)).astype(BF16)

    each_head(far_grads)
    drain(facs_ref.at[pl.ds(0, n - 1)], fac_sems.at[0])
    for part in range(parts):
        for phase, buffer in ((0, send1), (2, out1), (3, send2), (5, out2)):
            drain(others(buffer, part), send_sems.at[phase, part])
        drain(agg1.at[part, half], send_sems.at[1, part])
        drain(agg2.at[part, half], send_sems.at[4, part])


def store(*refs):
    sources, targets, sems = refs[:4], refs[4:8], refs[8]
    copies = [pltpu.make_async_copy(s, t, sems.at[at]) for at, (s, t) in enumerate(zip(sources, targets))]
    for copy in copies:
        copy.start()
    for copy in copies:
        copy.wait()


def body(outer_size, inner_size, query_rows, key_rows, value_rows, log_decay, grad_out):
    n = outer_size * inner_size
    heads, tokens = log_decay.shape
    wide = query_rows.shape[1]
    size = wide // heads
    count = n // 2
    chunk = heads * size // count
    parts = PARTS if chunk % (8 * PARTS) == 0 else 1
    rows = chunk // parts
    pieces = pltpu.VMEM((parts, count, rows, size), F32)
    sums = pltpu.VMEM((parts, 2, outer_size, rows, size), F32)
    vmem = pl.BlockSpec(memory_space=pltpu.VMEM)
    hbm = pl.BlockSpec(memory_space=pltpu.HBM)
    row_block = pltpu.VMEM((tokens, wide), BF16)
    outs = [jax.ShapeDtypeStruct((tokens, wide), BF16)] * 4
    results = pl.pallas_call(
        functools.partial(kernel, outer_size, inner_size, parts),
        out_shape=outs,
        in_specs=[hbm] * 5,
        out_specs=[vmem] * 4,
        scratch_shapes=[
            row_block, row_block, row_block, pltpu.VMEM((heads, tokens), F32), row_block,
            pltpu.VMEM((heads, tokens), F32),
            pltpu.VMEM((heads, tokens, size), F32),
            pltpu.VMEM((heads, 1, size), F32),
            pltpu.VMEM((heads, 1, size), F32),
            pltpu.VMEM((n, 1, size), F32),
            pltpu.VMEM((heads, tokens, tokens), F32),
            pltpu.VMEM((heads, tokens, tokens), BF16),
            row_block,
            pltpu.VMEM((tokens, wide), F32),
            row_block,
            pieces, pieces, pieces, pieces, sums, pieces, pieces, pieces, pieces, sums,
            pltpu.VMEM((heads, size, size), BF16),
            pltpu.VMEM((tokens, wide), F32),
            pltpu.VMEM((tokens, wide), F32),
            pltpu.SemaphoreType.DMA((5,)),
            pltpu.SemaphoreType.DMA((2,)),
            pltpu.SemaphoreType.DMA((6, parts)),
            pltpu.SemaphoreType.DMA((6, parts)),
        ],
        compiler_params=pltpu.CompilerParams(
            collective_id=0, has_side_effects=True, vmem_limit_bytes=40 * 1024 * 1024),
    )(*[pltpu.with_memory_space_constraint(x, pltpu.HBM) for x in (query_rows, key_rows, value_rows, log_decay, grad_out)])
    return pl.pallas_call(
        store,
        out_shape=outs,
        in_specs=[vmem] * 4,
        out_specs=[hbm] * 4,
        scratch_shapes=[pltpu.SemaphoreType.DMA((4,))],
        compiler_params=pltpu.CompilerParams(vmem_limit_bytes=8 * 1024 * 1024),
    )(*results)


def solution(mesh):
    both = ("outer", "inner")
    row_spec = P(both, None)
    return jax.shard_map(
        functools.partial(body, mesh.shape["outer"], mesh.shape["inner"]),
        mesh=mesh,
        in_specs=(row_spec, row_spec, row_spec, P(None, both), row_spec),
        out_specs=(row_spec,) * 4,
        check_vma=False,
    )
```
